32 devices in a mesh: section: 2 (over core), expert: 16 (over z, y, x).
Axes of the slice: x: 2, y: 2, z: 4, core: 2. Of those that a mesh axis runs over, the one named last changes fastest.
Arguments:
- grad_out: bfloat16 [2, 2048, 4096], P('section', 'expert'), may hold values from -6 to 6
- saved_hidden: bfloat16 [2, 2048, 8, 1024], P('section', 'expert'), may hold values from -6 to 6
- routes: int32 [2, 2048, 8], P('section', 'expert'), may hold values from 0 to 15, all different within a row; in each aligned block of 128 rows (0 to 127, 128 to 255, ..., all dimensions but the last counted through in order) at most 96 rows name the same one
- scores: float32 [2, 2048, 8], P('section', 'expert'), may hold values from 0.02 to 0.98
- down_weight: bfloat16 [2, 16, 1024, 4096], P('section', 'expert'), may hold values from -0.1875 to 0.1875
- router: bfloat16 [2, 16, 4096], P('section'), may hold values from -0.59765625 to 0.59765625
Outputs:
- weight_grad: bfloat16 [2, 16, 1024, 4096], P('section', 'expert')
- handed: bfloat16 [2, 2048, 4096], P('section', 'expert')
The draws below stay inside these ranges and needn't reach their ends.
Inputs may be any that keep to these rules, and one draw needn't show every extreme that they name: `routes`: each token names 8 different experts. Among the 128 tokens of one index of expert (aligned blocks), no expert is named more than 96 times, and in every draw some expert is named exactly 96 times in some block.
All inputs are finite; a program needn't handle non-finite values.
Results may differ from the reference program's by a relative error of at most 0.007.
Values may be sent and summed in bfloat16 or wider, within the bound.
A program may use at most 128 MiB of HBM per device.

```python
import math
import jax
import jax.numpy as jnp
import numpy as np
from jax import lax

D = 4096
FF = 1024
TOP = 8
TOK_DEV = 128
SECTIONS = 2
EXPERTS = 16
TOKENS = 2048
CAP = 96


def levels(stream_key, dims, shards, smallest, high):
    gain, own = 1.0, jax.random.fold_in(stream_key, 6)
    for axis_at, shards_of in shards:
        heights = jnp.exp(jax.random.uniform(jax.random.fold_in(own, axis_at), (shards_of,), jnp.float32, smallest / len(shards), high / len(shards)))
        gain = gain * jnp.repeat(heights, dims[axis_at] // shards_of).reshape([-1 if axis == axis_at else 1 for axis in range(len(dims))])
    return gain


def deal_out(stream_key, own, number, rows, amount, top, bound, skew):
    sequence = jax.random.permutation(stream_key, amount)
    packed, ordinary = load_shares(amount, rows * top, bound, skew, True), load_shares(amount, rows * top, bound, skew, False)
    places = jnp.arange(amount)

    def named(lengths, offset_by):
        used = int((lengths > 0).sum())
        fixed = max(1, used // 4)
        moved = fixed + (places - fixed + offset_by * (used - fixed)) % max(1, amount - fixed)
        return jnp.zeros((amount,), jnp.int32).at[sequence[jnp.where(places < fixed, places, moved)]].set(jnp.asarray(lengths, jnp.int32))

    lengths = jnp.where(number % 4 == 0, named(packed, number // 4), named(ordinary, number - number // 4 - 1))
    mixed = jax.random.permutation(jax.random.fold_in(own, 3), amount)
    source_of, sink = mixed[0:amount // 2 * 2:2], mixed[1:amount // 2 * 2:2]
    room = jnp.minimum(lengths[source_of] - 1, bound - lengths[sink]) // 2
    room = jnp.where((source_of == sequence[0]) | (sink == sequence[0]) | (lengths[sink] == 0), 0, jnp.maximum(room, 0))
    moved = jax.random.randint(jax.random.fold_in(own, 4), (amount // 2,), 0, 1 << 20) % (room + 1)
    lengths = lengths.at[source_of].add(-moved).at[sink].add(moved)
    items = jnp.searchsorted(jnp.cumsum(lengths), jnp.arange(rows * top), side="right").astype(jnp.int32)
    table = items.reshape(top, rows).T
    table = table[jax.random.permutation(jax.random.fold_in(own, 1), rows)]
    offset_by = jax.random.randint(jax.random.fold_in(own, 2), (rows, 1), 0, top)
    return jnp.take_along_axis(table, (jnp.arange(top)[None, :] + offset_by) % top, axis=1)


def load_shares(count, total, most, slope, full):
    portions = [(1 << 20) // math.isqrt(grade ** slope) + 1 for grade in range(1, count + 1)]
    largest = most if full else min(most, max(-(-total // count), total * portions[0] // sum(portions)))
    least = 1 if total - largest >= count - 1 else 0
    holding, rest = [largest] + [least] * (count - 1), total - largest - least * (count - 1)
    while rest > 0:
        free = [i for i in range(1, count) if holding[i] < largest] or [i for i in range(1, count) if holding[i] < most]
        mass, budget = sum([portions[i] for i in free]), rest
        for i in free:
            extra = min(most - holding[i], max(1, budget * portions[i] // mass), rest)
            holding[i] = holding[i] + extra
            rest = rest - extra
    return np.array(holding)


def centred(own_key, extent, width, most, shards=(), kind=jnp.bfloat16):
    result = jax.random.normal(own_key, extent, jnp.float32) * width
    if len(shards) > 0:
        result = levels(own_key, extent, shards, -0.22, 0.18) * result
    return jnp.clip(result, min=-most, max=most).astype(kind)


def setup_inputs(seed: int = 0) -> dict:
    key_of = jax.random.split(jax.random.key(seed), 7)
    grad_out = centred(key_of[0], (SECTIONS, TOKENS, D), 1.0, 6.0, ((0, 2), (1, 16)))
    saved_hidden = centred(key_of[1], (SECTIONS, TOKENS, TOP, FF), 1.0, 6.0, ((0, 2), (1, 16)))
    routes_keys = jax.random.split(jax.random.fold_in(key_of[2], 1), SECTIONS * TOKENS // TOK_DEV)
    routes_turns = jax.random.permutation(jax.random.fold_in(key_of[2], 3), SECTIONS * TOKENS // TOK_DEV)
    routes = jax.vmap(lambda own, number: deal_out(jax.random.fold_in(key_of[2], 2), own, number, TOK_DEV, EXPERTS, TOP, CAP, 2))(routes_keys, routes_turns).reshape((SECTIONS, TOKENS, TOP))
    scores = jnp.clip(0.02 + 0.96000002 * jax.random.uniform(key_of[3], (SECTIONS, TOKENS, TOP), jnp.float32) ** levels(key_of[3], (SECTIONS, TOKENS, TOP), ((0, 2), (1, 16)), -0.2, 0.2), 0.02, 0.98)
    down_weight = centred(key_of[4], (SECTIONS, EXPERTS, FF, D), FF ** -0.5, 0.1875, ((0, 2), (1, 16)))
    router = centred(key_of[5], (SECTIONS, EXPERTS, D), 0.1, 0.59765625, ((0, 2),))
    return dict(grad_out=grad_out, saved_hidden=saved_hidden, routes=routes, scores=scores, down_weight=down_weight, router=router)


def slot_rows(route_ids, n_experts, per_block, capacity):
    flat_routes = route_ids.reshape(-1)
    entries = flat_routes.shape[0]
    n_blocks = entries // per_block
    onehot = (flat_routes[:, None] == jnp.arange(n_experts, dtype=jnp.int32)[None, :]).astype(jnp.int32)
    running = jnp.cumsum(onehot.reshape(n_blocks, per_block, n_experts), axis=1).astype(jnp.int32)
    running = running.reshape(entries, n_experts)
    slot_index = jnp.sum(running * onehot, axis=1).astype(jnp.int32) - 1
    block_index = jnp.arange(entries, dtype=jnp.int32) // per_block
    row_index = (block_index * capacity + slot_index).astype(jnp.int32)
    source = jnp.full((n_experts, n_blocks * capacity), entries, jnp.int32)
    source = source.at[flat_routes, row_index].set(jnp.arange(entries, dtype=jnp.int32))
    return flat_routes, row_index, source


def section_pass(grad_rows, hidden_rows, route_ids, score_rows, down_all, router_rows):
    n_tokens, n_routes = route_ids.shape
    n_experts = router_rows.shape[0]
    entries = n_tokens * n_routes
    flat_routes, row_index, source = slot_rows(route_ids, n_experts, TOK_DEV * n_routes, CAP)
    score_total = jnp.sum(score_rows, axis=1, keepdims=True)
    weights = score_rows / score_total
    weights_low = weights.astype(jnp.bfloat16).reshape(-1)
    hidden_flat = hidden_rows.reshape(entries, hidden_rows.shape[2])

    def one_expert(operands):
        slot_source, expert_down = operands
        filled = slot_source < entries
        safe_index = jnp.minimum(slot_source, entries - 1)
        grad_in = jnp.where(filled[:, None], grad_rows[safe_index // n_routes], jnp.zeros((), jnp.bfloat16))
        hidden_in = jnp.where(filled[:, None], hidden_flat[safe_index], jnp.zeros((), jnp.bfloat16))
        weight_in = jnp.where(filled, weights_low[safe_index], jnp.zeros((), jnp.bfloat16))
        projected = lax.dot_general(grad_in, expert_down, (((1,), (1,)), ((), ())), preferred_element_type=jnp.float32)
        derivs = jnp.sum(projected * hidden_in.astype(jnp.float32), axis=1)
        scaled = (weight_in.astype(jnp.float32)[:, None] * grad_in.astype(jnp.float32)).astype(jnp.bfloat16)
        weight_grads = lax.dot_general(hidden_in, scaled, (((0,), (0,)), ((), ())), preferred_element_type=jnp.float32)
        return weight_grads.astype(jnp.bfloat16), derivs

    weight_grads, derivs = lax.map(one_expert, (source, down_all))
    derivs_home = derivs[flat_routes, row_index].reshape(n_tokens, n_routes)
    center = jnp.sum(weights * derivs_home, axis=1, keepdims=True)
    logit_grad = score_rows * (1.0 - score_rows) / score_total * (derivs_home - center)
    expert_ids = jnp.arange(n_experts, dtype=jnp.int32)
    dense_grad = jnp.sum(jnp.where(route_ids[:, :, None] == expert_ids[None, None, :], logit_grad[:, :, None], 0.0), axis=1)
    input_grad = grad_rows.astype(jnp.float32) + jnp.dot(dense_grad, router_rows.astype(jnp.float32), precision=lax.Precision.HIGHEST)
    return weight_grads, input_grad.astype(jnp.bfloat16)


def reference(grad_out, saved_hidden, routes, scores, down_weight, router):
    weight_list = []
    input_list = []
    for section_index in range(SECTIONS):
        weight_grads, input_grad = section_pass(grad_out[section_index], saved_hidden[section_index], routes[section_index], scores[section_index], down_weight[section_index], router[section_index])
        weight_list.append(weight_grads)
        input_list.append(input_grad)
    handed = jnp.roll(jnp.stack(input_list), -1, axis=0)
    return jnp.stack(weight_list), handed
```

```python
import functools

import jax
import jax.numpy as jnp
from jax import lax
from jax.experimental import pallas as pl
from jax.experimental.pallas import tpu as pltpu
from jax.sharding import PartitionSpec as P

MESH = pl.DeviceIdType.MESH


def torus_dims(n):
    dims = [1, 1, 1]
    at = 0
    while n > 1:
        factor = next(f for f in range(2, n + 1) if n % f == 0)
        dims[at % 3] *= factor
        n //= factor
        at += 1
    return tuple(dims)


def tree_edges(dims, order, flip):
    reached = [(0, 0, 0)]
    edges = []
    for axis in order:
        size = dims[axis]
        fresh = []
        for count, start in enumerate(reached):
            extra = (count + flip) % 2 if size % 2 == 0 else 0
            plus = (size - 1) // 2 + (1 - extra if size > 2 and size % 2 == 0 else 0)
            if size == 2:
                plus = 1
            minus = size - 1 - plus
            for step, hops in ((1, plus), (-1, minus)):
                place = start
                for _ in range(hops):
                    after = list(place)
                    after[axis] = (after[axis] + step) % size
                    after = tuple(after)
                    edges.append((place, axis, step, after))
                    fresh.append(after)
                    place = after
        reached = reached + fresh
    return edges


def plan(dims, orders):
    waiting = []
    for chunk, (order, flip) in enumerate(orders):
        edges = tree_edges(dims, order, flip)
        below = {}
        for parent, axis, step, child in reversed(edges):
            below[parent] = max(below.get(parent, 0), below.get(child, 0) + 1)
        for parent, axis, step, child in edges:
            waiting.append((chunk, parent, axis, step, child, below.get(child, 0)))
    arrival = {(chunk, (0, 0, 0)): 0 for chunk in range(len(orders))}
    free = {}
    issued = []
    while waiting:
        best = None
        for item in waiting:
            chunk, parent, axis, step, child, depth = item
            if (chunk, parent) not in arrival:
                continue
            begin = max(arrival[(chunk, parent)], free.get((axis, step), 0))
            key = (begin, -depth, chunk)
            if best is None or key < best[0]:
                best = (key, item)
        (begin, _, _), item = best
        waiting.remove(item)
        chunk, parent, axis, step, child, depth = item
        free[(axis, step)] = begin + 1
        arrival[(chunk, child)] = begin + 1.5
        issued.append((begin, item[:5]))
    issued.sort(key=lambda pair: pair[0])
    return [item for _, item in issued]


def flat(offset, dims):
    return (offset[0] * dims[1] + offset[1]) * dims[2] + offset[2]


def exchange_kernel(dims, sends, grad_ref, dense_ref, all_ref, got_ref, own, own_dense, g_send, g_recv, h_send, h_recv, local):
    n = dims[0] * dims[1] * dims[2]
    me = lax.axis_index("expert")
    here = (me // (dims[1] * dims[2]), (me // dims[2]) % dims[1], me % dims[2])

    def at(offset, sign):
        c = [(here[i] + sign * offset[i] + dims[i]) % dims[i] for i in range(3)]
        return (c[0] * dims[1] + c[1]) * dims[2] + c[2]

    load = pltpu.make_async_copy(grad_ref, own, local.at[0])
    load.start()
    load_dense = pltpu.make_async_copy(dense_ref.at[me], own_dense, local.at[1])
    load_dense.start()
    barrier = pltpu.get_barrier_semaphore()
    for i in range(1, n):
        pl.semaphore_signal(barrier, inc=1, device_id={"expert": (me + i) % n}, device_id_type=MESH)
    pl.semaphore_wait(barrier, n - 1)
    load.wait()

    offsets = [(a, b, c) for a in range(dims[0]) for b in range(dims[1]) for c in range(dims[2])]
    offsets = [o for o in offsets if o != (0, 0, 0)]

    def dense_copy(offset):
        k = flat(offset, dims)
        return pltpu.make_async_remote_copy(
            src_ref=dense_ref.at[at(offset, 1)],
            dst_ref=got_ref.at[me],
            send_sem=h_send.at[k],
            recv_sem=h_recv.at[k],
            device_id={"expert": at(offset, 1)},
            device_id_type=MESH,
        )

    def grad_copy(item):
        chunk, parent, axis, step, child = item
        source = at(parent, -1)
        move = [0, 0, 0]
        move[axis] = step
        k = flat(child, dims)
        return pltpu.make_async_remote_copy(
            src_ref=own.at[chunk] if parent == (0, 0, 0) else all_ref.at[source, chunk],
            dst_ref=all_ref.at[source, chunk],
            send_sem=g_send.at[k, chunk],
            recv_sem=g_recv.at[k, chunk],
            device_id={"expert": at(move, 1)},
            device_id_type=MESH,
        )

    def arrived(chunk, offset):
        k = flat(offset, dims)
        source = at(offset, -1)
        pltpu.make_async_copy(all_ref.at[source, chunk], all_ref.at[source, chunk], g_recv.at[k, chunk]).wait()

    seen = set()
    pending = list(offsets)
    copies = []
    dense_copies = []
    stores = []
    own_sends = sum(1 for item in sends if item[1] == (0, 0, 0))
    every = max(1, (len(sends) * 2 // 3 - own_sends) // max(1, len(pending)))
    for count, item in enumerate(sends):
        chunk, parent = item[0], item[1]
        if parent != (0, 0, 0) and (chunk, parent) not in seen:
            arrived(chunk, parent)
            seen.add((chunk, parent))
        copy = grad_copy(item)
        copy.start()
        copies.append(copy)
        if count >= own_sends and (count - own_sends) % every == 0 and pending:
            extra = dense_copy(pending.pop(0))
            extra.start()
            dense_copies.append(extra)
        if count == own_sends:
            store = pltpu.make_async_copy(own, all_ref.at[me], local.at[2])
            store.start()
            load_dense.wait()
            store_dense = pltpu.make_async_copy(own_dense, got_ref.at[me], local.at[3])
            store_dense.start()
            stores = [store, store_dense]
    for offset in pending:
        extra = dense_copy(offset)
        extra.start()
        dense_copies.append(extra)
    for offset in offsets:
        for chunk in range(own.shape[0]):
            if (chunk, offset) not in seen:
                arrived(chunk, offset)
    for copy in dense_copies:
        copy.wait_recv()
    for copy in dense_copies:
        copy.wait_send()
    for copy in copies:
        copy.wait_send()
    for store in stores:
        store.wait()


def exchange(grad_rows, dense):
    n, n_tokens, hidden_width = dense.shape
    width = grad_rows.shape[1]
    dims = torus_dims(n)
    orders = [((2, 1, 0), 0), ((1, 2, 0), 1), ((0, 2, 1), 0), ((0, 1, 2), 1)]
    chunks = len(orders)
    rows = n_tokens // chunks
    grad_chunks = grad_rows.reshape(chunks, rows, width)
    got, dense_got = pl.pallas_call(
        functools.partial(exchange_kernel, dims, plan(dims, orders)),
        out_shape=(
            jax.ShapeDtypeStruct((n, chunks, rows, width), grad_rows.dtype),
            jax.ShapeDtypeStruct(dense.shape, dense.dtype),
        ),
        in_specs=[pl.BlockSpec(memory_space=pl.ANY)] * 2,
        out_specs=(pl.BlockSpec(memory_space=pl.ANY), pl.BlockSpec(memory_space=pl.ANY)),
        scratch_shapes=[
            pltpu.VMEM((chunks, rows, width), grad_rows.dtype),
            pltpu.VMEM((n_tokens, hidden_width), dense.dtype),
            pltpu.SemaphoreType.DMA((n, chunks)),
            pltpu.SemaphoreType.DMA((n, chunks)),
            pltpu.SemaphoreType.DMA((n,)),
            pltpu.SemaphoreType.DMA((n,)),
            pltpu.SemaphoreType.DMA((4,)),
        ],
        compiler_params=pltpu.CompilerParams(collective_id=0, has_side_effects=True),
        name="exchange",
    )(grad_chunks, dense)
    return got.reshape(n * n_tokens, width), dense_got.reshape(n * n_tokens, hidden_width)


def spread_kernel(n_experts, group, top, hidden_ref, weight_ref, route_ref, out_ref):
    rows, cols = n_experts * group, group * top
    row = lax.broadcasted_iota(jnp.int32, (rows, cols), 0)
    col = lax.broadcasted_iota(jnp.int32, (rows, cols), 1)
    named = (row % group == col // top) & (row // group == route_ref[0])
    mix = jnp.where(named, weight_ref[0], 0.0).astype(jnp.bfloat16)
    for e in range(n_experts):
        part = jnp.dot(
            mix[e * group : (e + 1) * group], hidden_ref[...], preferred_element_type=jnp.float32
        )
        out_ref[e] = part.astype(jnp.bfloat16)


def spread(hidden_rows, weights_low, route_ids, n_experts):
    n_tokens, top, width = hidden_rows.shape
    group = 16
    steps = n_tokens // group
    cols = group * top
    return pl.pallas_call(
        functools.partial(spread_kernel, n_experts, group, top),
        grid=(steps,),
        out_shape=jax.ShapeDtypeStruct((n_experts, n_tokens, width), jnp.bfloat16),
        in_specs=[
            pl.BlockSpec((cols, width), lambda i: (i, 0)),
            pl.BlockSpec((1, 1, cols), lambda i: (i, 0, 0)),
            pl.BlockSpec((1, 1, cols), lambda i: (i, 0, 0)),
        ],
        out_specs=pl.BlockSpec((n_experts, group, width), lambda i: (0, i, 0)),
        name="spread",
    )(
        hidden_rows.reshape(n_tokens * top, width),
        weights_low.astype(jnp.float32).reshape(steps, 1, cols),
        route_ids.reshape(steps, 1, cols),
    )


def deriv_kernel(grad_ref, hidden_ref, down_ref, out_ref):
    projected = lax.dot_general(
        grad_ref[...], down_ref[...], (((1,), (1,)), ((), ())), preferred_element_type=jnp.float32
    )
    out_ref[...] = jnp.sum(projected * hidden_ref[...].astype(jnp.float32), axis=1, keepdims=True)


def derivs_of(grads, hidden, down):
    rows, width = grads.shape
    hidden_width = hidden.shape[1]
    tile = 512
    return pl.pallas_call(
        deriv_kernel,
        grid=(rows // tile,),
        out_shape=jax.ShapeDtypeStruct((rows, 1), jnp.float32),
        in_specs=[
            pl.BlockSpec((tile, width), lambda i: (i, 0)),
            pl.BlockSpec((tile, hidden_width), lambda i: (i, 0)),
            pl.BlockSpec((hidden_width, width), lambda i: (0, 0)),
        ],
        out_specs=pl.BlockSpec((tile, 1), lambda i: (i, 0)),
        compiler_params=pltpu.CompilerParams(vmem_limit_bytes=50 * 1024 * 1024),
        cost_estimate=pl.CostEstimate(
            flops=2 * rows * width * hidden_width, bytes_accessed=2 * rows * width, transcendentals=0
        ),
        name="derivs",
    )(grads, hidden, down)


def passed_along(array, axis, by):
    size = lax.axis_size(axis)
    return lax.ppermute(array, axis, [(i, (i + by) % size) for i in range(size)])


def body(grad_out, saved_hidden, routes, scores, down_weight, router):
    grad_rows = grad_out[0]
    hidden_rows = saved_hidden[0]
    route_ids = routes[0]
    score_rows = scores[0]
    n_tokens = grad_rows.shape[0]
    n_experts = router.shape[1]
    score_total = jnp.sum(score_rows, axis=1, keepdims=True)
    weights = score_rows / score_total
    weights_low = weights.astype(jnp.bfloat16)

    next_grad = passed_along(grad_rows, "section", -1)
    next_router = passed_along(router[0], "section", -1)
    dense = spread(hidden_rows, weights_low, route_ids, n_experts)
    grads, hidden = exchange(grad_rows, dense)
    derivs = derivs_of(grads, hidden, down_weight[0, 0])
    home = lax.all_to_all(
        derivs.reshape(n_experts, n_tokens), "expert", split_axis=0, concat_axis=0, tiled=True
    )
    weight_out = lax.dot_general(
        hidden, grads, (((0,), (0,)), ((), ())), preferred_element_type=jnp.float32
    ).astype(jnp.bfloat16)

    named = route_ids.T[None] == jnp.arange(n_experts, dtype=jnp.int32)[:, None, None]
    low = weights_low.astype(jnp.float32)
    score_dense = jnp.sum(jnp.where(named, score_rows.T[None], 0.0), axis=1)
    fix_dense = jnp.sum(jnp.where(named, (weights / low).T[None], 0.0), axis=1)
    weighted = home * fix_dense
    center = jnp.sum(weighted, axis=0, keepdims=True)
    total_row = score_total.T
    logit_dense = (1.0 - score_dense) * (weighted - score_dense / total_row * center)
    next_logit = passed_along(logit_dense, "section", -1)
    handed = next_grad.astype(jnp.float32) + lax.dot_general(
        next_logit,
        next_router.astype(jnp.float32),
        (((0,), (0,)), ((), ())),
        precision=lax.Precision.HIGHEST,
    )
    return (weight_out[None, None], handed.astype(jnp.bfloat16)[None])


def solution(mesh):
    return jax.shard_map(
        body,
        mesh=mesh,
        in_specs=(
            P("section", "expert", None),
            P("section", "expert", None, None),
            P("section", "expert", None),
            P("section", "expert", None),
            P("section", "expert", None, None),
            P("section", None, None),
        ),
        out_specs=(P("section", "expert", None, None), P("section", "expert", None)),
        check_vma=False,
    )
```

```python
import functools

import jax
import jax.numpy as jnp
from jax import lax
from jax.experimental import pallas as pl
from jax.experimental.pallas import tpu as pltpu
from jax.sharding import PartitionSpec as P

MESH = pl.DeviceIdType.MESH


def torus_dims(n):
    dims = [1, 1, 1]
    at = 0
    while n > 1:
        factor = next(f for f in range(2, n + 1) if n % f == 0)
        dims[at % 3] *= factor
        n //= factor
        at += 1
    return tuple(dims)


def tree_edges(dims, order, flip):
    reached = [(0, 0, 0)]
    edges = []
    for axis in order:
        size = dims[axis]
        fresh = []
        for count, start in enumerate(reached):
            extra = (count + flip) % 2 if size % 2 == 0 else 0
            plus = (size - 1) // 2 + (1 - extra if size > 2 and size % 2 == 0 else 0)
            if size == 2:
                plus = 1
            minus = size - 1 - plus
            for step, hops in ((1, plus), (-1, minus)):
                place = start
                for _ in range(hops):
                    after = list(place)
                    after[axis] = (after[axis] + step) % size
                    after = tuple(after)
                    edges.append((place, axis, step, after))
                    fresh.append(after)
                    place = after
        reached = reached + fresh
    return edges


def plan(dims, orders):
    waiting = []
    for chunk, (order, flip) in enumerate(orders):
        edges = tree_edges(dims, order, flip)
        below = {}
        for parent, axis, step, child in reversed(edges):
            below[parent] = max(below.get(parent, 0), below.get(child, 0) + 1)
        for parent, axis, step, child in edges:
            waiting.append((chunk, parent, axis, step, child, below.get(child, 0)))
    arrival = {(chunk, (0, 0, 0)): 0 for chunk in range(len(orders))}
    free = {}
    issued = []
    while waiting:
        best = None
        for item in waiting:
            chunk, parent, axis, step, child, depth = item
            if (chunk, parent) not in arrival:
                continue
            begin = max(arrival[(chunk, parent)], free.get((axis, step), 0))
            key = (begin, -depth, chunk)
            if best is None or key < best[0]:
                best = (key, item)
        (begin, _, _), item = best
        waiting.remove(item)
        chunk, parent, axis, step, child, depth = item
        free[(axis, step)] = begin + 1
        arrival[(chunk, child)] = begin + 1.5
        issued.append((begin, item[:5]))
    issued.sort(key=lambda pair: pair[0])
    return [item for _, item in issued]


def flat(offset, dims):
    return (offset[0] * dims[1] + offset[1]) * dims[2] + offset[2]


def exchange_kernel(dims, sends, grad_ref, dense_ref, all_ref, got_ref, own, own_dense, g_send, g_recv, h_send, h_recv, local):
    n = dims[0] * dims[1] * dims[2]
    me = lax.axis_index("expert")
    here = (me // (dims[1] * dims[2]), (me // dims[2]) % dims[1], me % dims[2])

    def at(offset, sign):
        c = [(here[i] + sign * offset[i] + dims[i]) % dims[i] for i in range(3)]
        return (c[0] * dims[1] + c[1]) * dims[2] + c[2]

    load = pltpu.make_async_copy(grad_ref, own, local.at[0])
    load.start()
    load_dense = pltpu.make_async_copy(dense_ref.at[me], own_dense, local.at[1])
    load_dense.start()
    barrier = pltpu.get_barrier_semaphore()
    for i in range(1, n):
        pl.semaphore_signal(barrier, inc=1, device_id={"expert": (me + i) % n}, device_id_type=MESH)
    pl.semaphore_wait(barrier, n - 1)
    load.wait()

    offsets = [(a, b, c) for a in range(dims[0]) for b in range(dims[1]) for c in range(dims[2])]
    offsets = [o for o in offsets if o != (0, 0, 0)]

    def dense_copy(offset):
        k = flat(offset, dims)
        return pltpu.make_async_remote_copy(
            src_ref=dense_ref.at[at(offset, 1)],
            dst_ref=got_ref.at[me],
            send_sem=h_send.at[k],
            recv_sem=h_recv.at[k],
            device_id={"expert": at(offset, 1)},
            device_id_type=MESH,
        )

    def grad_copy(item):
        chunk, parent, axis, step, child = item
        source = at(parent, -1)
        move = [0, 0, 0]
        move[axis] = step
        k = flat(child, dims)
        return pltpu.make_async_remote_copy(
            src_ref=own.at[chunk] if parent == (0, 0, 0) else all_ref.at[source, chunk],
            dst_ref=all_ref.at[source, chunk],
            send_sem=g_send.at[k, chunk],
            recv_sem=g_recv.at[k, chunk],
            device_id={"expert": at(move, 1)},
            device_id_type=MESH,
        )

    def arrived(chunk, offset):
        k = flat(offset, dims)
        source = at(offset, -1)
        pltpu.make_async_copy(all_ref.at[source, chunk], all_ref.at[source, chunk], g_recv.at[k, chunk]).wait()

    seen = set()
    pending = list(offsets)
    copies = []
    dense_copies = []
    stores = []
    own_sends = sum(1 for item in sends if item[1] == (0, 0, 0))
    every = max(1, (len(sends) * 2 // 3 - own_sends) // max(1, len(pending)))
    for count, item in enumerate(sends):
        chunk, parent = item[0], item[1]
        if parent != (0, 0, 0) and (chunk, parent) not in seen:
            arrived(chunk, parent)
            seen.add((chunk, parent))
        copy = grad_copy(item)
        copy.start()
        copies.append(copy)
        if count >= own_sends and (count - own_sends) % every == 0 and pending:
            extra = dense_copy(pending.pop(0))
            extra.start()
            dense_copies.append(extra)
        if count == own_sends:
            store = pltpu.make_async_copy(own, all_ref.at[me], local.at[2])
            store.start()
            load_dense.wait()
            store_dense = pltpu.make_async_copy(own_dense, got_ref.at[me], local.at[3])
            store_dense.start()
            stores = [store, store_dense]
    for offset in pending:
        extra = dense_copy(offset)
        extra.start()
        dense_copies.append(extra)
    for offset in offsets:
        for chunk in range(own.shape[0]):
            if (chunk, offset) not in seen:
                arrived(chunk, offset)
    for copy in dense_copies:
        copy.wait_recv()
    for copy in dense_copies:
        copy.wait_send()
    for copy in copies:
        copy.wait_send()
    for store in stores:
        store.wait()


def line_kernel(dims, orders, grad_ref, dense_ref, all_ref, got_ref, own, own_dense, g_send, g_recv, h_send, h_recv, local):
    n = dims[0] * dims[1] * dims[2]
    chunks = len(orders)
    me = lax.axis_index("expert")
    here = [me // (dims[1] * dims[2]), (me // dims[2]) % dims[1], me % dims[2]]

    def number(c):
        return (c[0] * dims[1] + c[1]) * dims[2] + c[2]

    load = pltpu.make_async_copy(grad_ref, own, local.at[0])
    load.start()
    load_dense = pltpu.make_async_copy(dense_ref.at[me], own_dense, local.at[1])
    load_dense.start()
    barrier = pltpu.get_barrier_semaphore()
    for i in range(1, n):
        pl.semaphore_signal(barrier, inc=1, device_id={"expert": (me + i) % n}, device_id_type=MESH)
    pl.semaphore_wait(barrier, n - 1)
    load.wait()

    def start(source, chunk, axis, step, home):
        target = list(here)
        target[axis] = (here[axis] + step) % dims[axis]
        pltpu.make_async_remote_copy(
            src_ref=own.at[chunk] if home else all_ref.at[source, chunk],
            dst_ref=all_ref.at[source, chunk],
            send_sem=g_send.at[source, chunk, axis, (step + 1) // 2],
            recv_sem=g_recv.at[source, chunk],
            device_id={"expert": number(target)},
            device_id_type=MESH,
        ).start()

    def finish(source, chunk, axis, step, home):
        piece = own.at[chunk] if home else all_ref.at[source, chunk]
        pltpu.make_async_copy(piece, piece, g_send.at[source, chunk, axis, (step + 1) // 2]).wait()

    def moves(offset, order):
        last = max([i for i in range(3) if offset[order[i]] != 0], default=-1)
        steps = []
        if last >= 0 and dims[order[last]] > 2:
            steps.append((order[last], 1 if offset[order[last]] > 0 else -1))
        for axis in order[last + 1 :]:
            if dims[axis] == 2:
                steps.append((axis, 1))
            elif dims[axis] > 2:
                steps += [(axis, 1), (axis, -1)]
        return steps

    def each_move(offset, order, chunk, act):
        source = number([(here[i] - offset[i] + dims[i]) % dims[i] for i in range(3)])
        home = offset == (0, 0, 0)
        for axis, step in moves(offset, order):
            if dims[axis] == 2:
                act(source, chunk, axis, step, home)
            else:
                inside = here[axis] < dims[axis] - 1 if step > 0 else here[axis] > 0
                pl.when(inside)(functools.partial(act, source, chunk, axis, step, home))

    def on_slice(offset, act):
        valid = None
        for i in range(3):
            if dims[i] > 2 and offset[i] != 0:
                inside = here[i] >= offset[i] if offset[i] > 0 else here[i] < dims[i] + offset[i]
                valid = inside if valid is None else valid & inside
        if valid is None:
            act()
        else:
            pl.when(valid)(act)

    spans = [range(size) if size <= 2 else range(1 - size, size) for size in dims]
    offsets = [(a, b, c) for a in spans[0] for b in spans[1] for c in spans[2] if (a, b, c) != (0, 0, 0)]

    for chunk in range(chunks):
        each_move((0, 0, 0), orders[chunk], chunk, start)

    def dense_copy(k):
        return pltpu.make_async_remote_copy(
            src_ref=dense_ref.at[(me + k) % n],
            dst_ref=got_ref.at[me],
            send_sem=h_send.at[k],
            recv_sem=h_recv.at[k],
            device_id={"expert": (me + k) % n},
            device_id_type=MESH,
        )

    store = pltpu.make_async_copy(own, all_ref.at[me], local.at[2])
    store.start()
    load_dense.wait()
    store_dense = pltpu.make_async_copy(own_dense, got_ref.at[me], local.at[3])
    store_dense.start()

    arrivals = []
    for chunk in range(chunks):
        for offset in offsets:
            hops = [abs(offset[axis]) for axis in orders[chunk]]
            arrivals.append((hops[0] * WEIGHTS[0] + hops[1] * WEIGHTS[1] + hops[2] * WEIGHTS[2], chunk, offset))
    arrivals.sort()
    far = sorted(range(1, n), key=lambda k: -min(k, n - k))
    every = max(1, (len(arrivals) * SHARE // 4) // len(far))
    for count, (_, chunk, offset) in enumerate(arrivals):
        if count % every == 0 and far:
            dense_copy(far.pop(0)).start()

        def arrive(chunk=chunk, offset=offset):
            source = number([(here[i] - offset[i] + dims[i]) % dims[i] for i in range(3)])
            piece = all_ref.at[source, chunk]
            pltpu.make_async_copy(piece, piece, g_recv.at[source, chunk]).wait()
            each_move(offset, orders[chunk], chunk, start)

        on_slice(offset, arrive)
    for k in far:
        dense_copy(k).start()
    for k in range(1, n):
        dense_copy(k).wait()
    for chunk in range(chunks):
        each_move((0, 0, 0), orders[chunk], chunk, finish)
        for offset in offsets:
            if moves(offset, orders[chunk]):
                on_slice(offset, functools.partial(each_move, offset, orders[chunk], chunk, finish))
    store.wait()
    store_dense.wait()


WEIGHTS = (2, 3, 3)
SHARE = 3
LINE_ORDERS = ((0, 2, 1), (0, 1, 2), (0, 2, 1), (0, 1, 2))


def exchange(grad_rows, dense):
    n, n_tokens, hidden_width = dense.shape
    width = grad_rows.shape[1]
    dims = torus_dims(n)
    on_line = 2 in dims
    orders = [((2, 1, 0), 0), ((1, 2, 0), 1), ((0, 2, 1), 0), ((0, 1, 2), 1)]
    if on_line:
        kernel, chunks = functools.partial(line_kernel, dims, LINE_ORDERS), len(LINE_ORDERS)
    else:
        kernel, chunks = functools.partial(exchange_kernel, dims, plan(dims, orders)), len(orders)
    rows = n_tokens // chunks
    grad_chunks = grad_rows.reshape(chunks, rows, width)
    got, dense_got = pl.pallas_call(
        kernel,
        out_shape=(
            jax.ShapeDtypeStruct((n, chunks, rows, width), grad_rows.dtype),
            jax.ShapeDtypeStruct(dense.shape, dense.dtype),
        ),
        in_specs=[pl.BlockSpec(memory_space=pl.ANY)] * 2,
        out_specs=(pl.BlockSpec(memory_space=pl.ANY), pl.BlockSpec(memory_space=pl.ANY)),
        scratch_shapes=[
            pltpu.VMEM((chunks, rows, width), grad_rows.dtype),
            pltpu.VMEM((n_tokens, hidden_width), dense.dtype),
            pltpu.SemaphoreType.DMA((n, chunks, 3, 2) if on_line else (n, chunks)),
            pltpu.SemaphoreType.DMA((n, chunks)),
            pltpu.SemaphoreType.DMA((n,)),
            pltpu.SemaphoreType.DMA((n,)),
            pltpu.SemaphoreType.DMA((4,)),
        ],
        compiler_params=pltpu.CompilerParams(collective_id=0, has_side_effects=True),
        name="exchange",
    )(grad_chunks, dense)
    return got.reshape(n * n_tokens, width), dense_got.reshape(n * n_tokens, hidden_width)


def spread_kernel(n_experts, group, top, hidden_ref, weight_ref, route_ref, out_ref):
    rows, cols = n_experts * group, group * top
    row = lax.broadcasted_iota(jnp.int32, (rows, cols), 0)
    col = lax.broadcasted_iota(jnp.int32, (rows, cols), 1)
    named = (row % group == col // top) & (row // group == route_ref[0])
    mix = jnp.where(named, weight_ref[0], 0.0).astype(jnp.bfloat16)
    for e in range(n_experts):
        part = jnp.dot(
            mix[e * group : (e + 1) * group], hidden_ref[...], preferred_element_type=jnp.float32
        )
        out_ref[e] = part.astype(jnp.bfloat16)


def spread(hidden_rows, weights_low, route_ids, n_experts):
    n_tokens, top, width = hidden_rows.shape
    group = 16
    steps = n_tokens // group
    cols = group * top
    return pl.pallas_call(
        functools.partial(spread_kernel, n_experts, group, top),
        grid=(steps,),
        out_shape=jax.ShapeDtypeStruct((n_experts, n_tokens, width), jnp.bfloat16),
        in_specs=[
            pl.BlockSpec((cols, width), lambda i: (i, 0)),
            pl.BlockSpec((1, 1, cols), lambda i: (i, 0, 0)),
            pl.BlockSpec((1, 1, cols), lambda i: (i, 0, 0)),
        ],
        out_specs=pl.BlockSpec((n_experts, group, width), lambda i: (0, i, 0)),
        name="spread",
    )(
        hidden_rows.reshape(n_tokens * top, width),
        weights_low.astype(jnp.float32).reshape(steps, 1, cols),
        route_ids.reshape(steps, 1, cols),
    )


def deriv_kernel(grad_ref, hidden_ref, down_ref, out_ref):
    projected = lax.dot_general(
        grad_ref[...], down_ref[...], (((1,), (1,)), ((), ())), preferred_element_type=jnp.float32
    )
    out_ref[...] = jnp.sum(projected * hidden_ref[...].astype(jnp.float32), axis=1, keepdims=True)


def derivs_of(grads, hidden, down):
    rows, width = grads.shape
    hidden_width = hidden.shape[1]
    tile = 512
    return pl.pallas_call(
        deriv_kernel,
        grid=(rows // tile,),
        out_shape=jax.ShapeDtypeStruct((rows, 1), jnp.float32),
        in_specs=[
            pl.BlockSpec((tile, width), lambda i: (i, 0)),
            pl.BlockSpec((tile, hidden_width), lambda i: (i, 0)),
            pl.BlockSpec((hidden_width, width), lambda i: (0, 0)),
        ],
        out_specs=pl.BlockSpec((tile, 1), lambda i: (i, 0)),
        compiler_params=pltpu.CompilerParams(vmem_limit_bytes=50 * 1024 * 1024),
        cost_estimate=pl.CostEstimate(
            flops=2 * rows * width * hidden_width, bytes_accessed=2 * rows * width, transcendentals=0
        ),
        name="derivs",
    )(grads, hidden, down)


def passed_along(array, axis, by):
    size = lax.axis_size(axis)
    return lax.ppermute(array, axis, [(i, (i + by) % size) for i in range(size)])


def body(grad_out, saved_hidden, routes, scores, down_weight, router):
    grad_rows = grad_out[0]
    hidden_rows = saved_hidden[0]
    route_ids = routes[0]
    score_rows = scores[0]
    n_tokens = grad_rows.shape[0]
    n_experts = router.shape[1]
    score_total = jnp.sum(score_rows, axis=1, keepdims=True)
    weights = score_rows / score_total
    weights_low = weights.astype(jnp.bfloat16)

    next_grad = passed_along(grad_rows, "section", -1)
    next_router = passed_along(router[0], "section", -1)
    dense = spread(hidden_rows, weights_low, route_ids, n_experts)
    grads, hidden = exchange(grad_rows, dense)
    derivs = derivs_of(grads, hidden, down_weight[0, 0])
    home = lax.all_to_all(
        derivs.reshape(n_experts, n_tokens), "expert", split_axis=0, concat_axis=0, tiled=True
    )
    weight_out = lax.dot_general(
        hidden, grads, (((0,), (0,)), ((), ())), preferred_element_type=jnp.float32
    ).astype(jnp.bfloat16)

    named = route_ids.T[None] == jnp.arange(n_experts, dtype=jnp.int32)[:, None, None]
    low = weights_low.astype(jnp.float32)
    score_dense = jnp.sum(jnp.where(named, score_rows.T[None], 0.0), axis=1)
    fix_dense = jnp.sum(jnp.where(named, (weights / low).T[None], 0.0), axis=1)
    weighted = home * fix_dense
    center = jnp.sum(weighted, axis=0, keepdims=True)
    total_row = score_total.T
    logit_dense = (1.0 - score_dense) * (weighted - score_dense / total_row * center)
    next_logit = passed_along(logit_dense, "section", -1)
    handed = next_grad.astype(jnp.float32) + lax.dot_general(
        next_logit,
        next_router.astype(jnp.float32),
        (((0,), (0,)), ((), ())),
        precision=lax.Precision.HIGHEST,
    )
    return (weight_out[None, None], handed.astype(jnp.bfloat16)[None])


def solution(mesh):
    return jax.shard_map(
        body,
        mesh=mesh,
        in_specs=(
            P("section", "expert", None),
            P("section", "expert", None, None),
            P("section", "expert", None),
            P("section", "expert", None),
            P("section", "expert", None, None),
            P("section", None, None),
        ),
        out_specs=(P("section", "expert", None, None), P("section", "expert", None)),
        check_vma=False,
    )
```
